32 devices in a mesh: band: 4 (over y, x), lev: 8 (over z, core).
Axes of the slice: x: 2, y: 2, z: 4, core: 2. Of those that a mesh axis runs over, the one named last changes fastest.
Arguments:
- adj_spec: bfloat16 [32, 1280, 2, 1280], P('lev', 'band'), may hold values from -6 to 6
- wave_of_slot: int32 [1280], replicated, may hold values from 0 to 1279, each once
- legendre: bfloat16 [1280, 8, 1280], P('band'), may hold values from -0.15625 to 0.15625
- lat_weight: float32 [8], replicated, may hold values from 0.5 to 1.5
- traj: bfloat16 [32, 16, 5136], P('lev', 'band'), may hold values from -3 to 3
- traj_exp: int32 [32, 16, 4], P('lev', 'band'), may hold values from -2 to 2
- traj_order: int32 [8, 4], P('lev'), may hold values from 0 to 3, each once within a row
- lev_coef: float32 [32], P('lev'), may hold values from 0.02 to 0.2
Outputs:
- adj_out: bfloat16 [32, 1280, 2, 1280], P('lev', 'band')
The draws below stay inside these ranges and needn't reach their ends.
Inputs may be any that keep to these rules, and one draw needn't show every extreme that they name: `wave_of_slot`: every wavenumber 0 to 1279 is held by exactly one slot. `traj_order`: each row is a permutation of 0 to 3.
All inputs are finite; a program needn't handle non-finite values.
Results may differ from the reference program's by a relative error of at most 0.0085.
Values may be sent and summed in bfloat16 or wider, within the bound.
A program may use at most 128 MiB of HBM per device.

```python
import math
import jax
import jax.numpy as jnp
from jax import lax

M = 1280
NLON = 5136
NBLK = 4
LEV_DEV = 4
NLAT = 16
NH = 8
NLEV = 32
N_LEV = 8


def touch_ends(values, key, smallest, largest):
    longest = values.shape.index(max(values.shape))
    spots = []
    for shift in (0, 1):
        where = [jax.random.randint(jax.random.fold_in(key, axis), (), 0, length) for axis, length in enumerate(values.shape)]
        where[longest] = (where[longest] + shift) % values.shape[longest]
        spots.append(tuple(where))
    return values.at[spots[0]].set(smallest).at[spots[1]].set(largest)


def levels(stream_key, shape, shards, smallest, top_value):
    loudness = 1.0
    for position, blocks in shards:
        steps = jax.random.uniform(jax.random.fold_in(jax.random.fold_in(stream_key, 6), position), (blocks,), jnp.float32, smallest / len(shards), top_value / len(shards))
        loudness = loudness * jnp.repeat(jnp.exp(steps), shape[position] // blocks).reshape((-1,) + (1,) * (len(shape) - 1 - position))
    return loudness


def noise(own_key, extent, width, bound, cuts=(), held_as=jnp.bfloat16):
    values = jax.random.normal(own_key, extent, jnp.float32) * width
    if len(cuts) > 0:
        values = levels(own_key, extent, cuts, -0.22, 0.18) * values
    return jnp.clip(values, min=-bound, max=bound).astype(held_as)


def setup_inputs(seed: int = 0) -> dict:
    key_list = jax.random.split(jax.random.key(seed), 9)
    adj_spec = noise(key_list[0], (NLEV, M, 2, M), 1.0, 6.0, ((0, 8), (1, 4)))
    wave_of_slot = jax.random.permutation(key_list[1], M).astype(jnp.int32)
    legendre = noise(key_list[2], (M, NH, M), M ** -0.5, 0.15625, ((0, 4),))
    lat_weight = jnp.clip(jax.random.uniform(key_list[3], (NH,), jnp.float32, 0.5, 1.5), 0.5, 1.5)
    traj = noise(key_list[4], (NLEV, NLAT, NLON), 0.5, 3.0, ((0, 8), (1, 4)))
    traj_exp = touch_ends(jax.random.randint(key_list[5], (NLEV, NLAT, NBLK), -2, 3), jax.random.fold_in(key_list[5], 1), -2, 2).astype(jnp.int32)
    traj_order = jax.vmap(lambda own: jax.random.permutation(own, LEV_DEV))(jax.random.split(key_list[6], N_LEV)).reshape((N_LEV, LEV_DEV)).astype(jnp.int32)
    lev_coef = jnp.clip(jnp.exp(math.log(0.2) - 2.3025851 * jax.random.uniform(key_list[7], (NLEV,), jnp.float32) ** levels(key_list[7], (NLEV,), ((0, 8),), -0.2, 0.2)), 0.02, 0.2)
    return {"adj_spec": adj_spec, "wave_of_slot": wave_of_slot, "legendre": legendre, "lat_weight": lat_weight, "traj": traj, "traj_exp": traj_exp, "traj_order": traj_order, "lev_coef": lev_coef}


def trig_block(wave_ids, lon_start, block_width, lon_count):
    lon_ids = lon_start + jnp.arange(block_width, dtype=jnp.int32)
    phase_int = wave_ids.astype(jnp.int32)[:, None] * lon_ids[None, :] % lon_count
    angle_rad = phase_int.astype(jnp.float32) * (2.0 * math.pi / lon_count)
    return jnp.stack([jnp.cos(angle_rad), -jnp.sin(angle_rad)], axis=1).astype(jnp.bfloat16)

def reference(adj_spec, wave_of_slot, legendre, lat_weight, traj, traj_exp, traj_order, lev_coef):
    highest = lax.Precision.HIGHEST
    degree_ids = jnp.arange(M, dtype=jnp.int32)
    valid_mask = degree_ids[None, :] < (M - wave_of_slot.astype(jnp.int32))[:, None]
    masked = jnp.where(valid_mask[None, :, None, :], adj_spec, jnp.zeros_like(adj_spec))
    parity_sign = jnp.where(degree_ids % 2 == 0, 1.0, -1.0).astype(jnp.float32)
    table_full = legendre.astype(jnp.float32)
    weight_q = jnp.repeat(lat_weight, 2)

    def synthesis(level_data):
        values = level_data.astype(jnp.float32)
        stacked = jnp.stack([values, values * parity_sign], axis=2)
        side_values = jnp.einsum('scej,shj->sche', stacked, table_full, precision=highest)
        return (side_values.reshape(M, 2, NLAT) * weight_q).astype(jnp.bfloat16)
    fourier = lax.map(synthesis, masked).astype(jnp.float32)
    block_width = NLON // NBLK
    norm_scale = 1.0 / math.sqrt(M)
    stored = traj.astype(jnp.float32).reshape(N_LEV, LEV_DEV, NLAT, NLON)
    select = (traj_order[:, None, :] == jnp.arange(LEV_DEV, dtype=jnp.int32)[None, :, None]).astype(jnp.float32)
    level_coef = lev_coef[:, None, None]
    analysis = jnp.zeros((NLEV, M, 2, NLAT), jnp.float32)
    for block_id in range(NBLK):
        lon_start = block_id * block_width
        trig_table = trig_block(wave_of_slot, lon_start, block_width, NLON).astype(jnp.float32)
        grid_block = jnp.einsum('lscq,scw->lqw', fourier, trig_table, precision=highest) * norm_scale
        running = jnp.cumsum(grid_block, axis=0)
        above_sum = jnp.concatenate([jnp.zeros_like(grid_block[:1]), running[:-1]], axis=0)
        exponent = jnp.exp2(traj_exp[:, :, block_id].astype(jnp.float32)).reshape(N_LEV, LEV_DEV, NLAT)
        traj_piece = stored[..., lon_start:lon_start + block_width] * exponent[..., None]
        traj_value = jnp.einsum('gir,grqw->giqw', select, traj_piece, precision=highest).reshape(NLEV, NLAT, block_width)
        forcing = ((1.0 + jnp.tanh(traj_value)) * (grid_block + level_coef * above_sum)).astype(jnp.bfloat16).astype(jnp.float32)
        analysis = analysis + jnp.einsum('lqw,scw->lscq', forcing, trig_table, precision=highest) * norm_scale
    halves = analysis.reshape(NLEV, M, 2, NH, 2)
    sym_part = (halves[..., 0] + halves[..., 1]).astype(jnp.bfloat16)
    anti_part = (halves[..., 0] - halves[..., 1]).astype(jnp.bfloat16)

    def analysis_level(level_pair):
        from_sym = jnp.einsum('sch,shj->scj', level_pair[0].astype(jnp.float32), table_full, precision=highest)
        from_anti = jnp.einsum('sch,shj->scj', level_pair[1].astype(jnp.float32), table_full, precision=highest)
        return jnp.where(degree_ids % 2 == 0, from_sym, from_anti)
    result = lax.map(analysis_level, (sym_part, anti_part))
    return jnp.where(valid_mask[None, :, None, :], result, 0.0).astype(jnp.bfloat16)
```

```python
import functools
import math

import jax
import jax.numpy as jnp
from jax import lax
from jax.experimental import pallas as pl
from jax.experimental.pallas import tpu as pltpu
from jax.sharding import PartitionSpec as P

NBLK = 4
LANES = 128


def slot_step(slots):
    step = 64 if slots % 64 == 0 else slots
    sub = next(width for width in (32, 16, 8, 4, 2, 1) if step % width == 0)
    return step, sub


def split_parity(leg_ref, limit_ref, first, sub):
    table = leg_ref[pl.ds(first, sub)].astype(jnp.float32)
    heights, degrees = table.shape[1], table.shape[2]
    lane = lax.broadcasted_iota(jnp.int32, table.shape, 2)
    limit = jnp.concatenate([limit_ref[pl.ds(first, sub)]] * (degrees // LANES), axis=2)
    table = jnp.where(lane < limit, table, 0.0)
    even = jnp.where(lane % 2 == 0, table, 0.0)
    odd = jnp.where(lane % 2 == 0, 0.0, table)
    rows = sub * heights
    return (
        even.reshape(rows, degrees).astype(jnp.bfloat16),
        odd.reshape(rows, degrees).astype(jnp.bfloat16),
    )


def same_slot(sub, heights, levels):
    shape = (sub, heights, levels * sub * 2)
    held = lax.broadcasted_iota(jnp.int32, shape, 0)
    lane = lax.broadcasted_iota(jnp.int32, shape, 2)
    return held == (lane % (sub * 2)) // 2


def swap_pairs(value):
    lane = lax.broadcasted_iota(jnp.int32, value.shape, 1)
    width = value.shape[1]
    return jnp.where(lane % 2 == 0, pltpu.roll(value, width - 1, 1), pltpu.roll(value, 1, 1))


def synthesis_kernel(step, sub, x_ref, leg_ref, limit_ref, weight_ref, turn_ref, out_ref):
    levels, degrees = x_ref.shape[0], x_ref.shape[3]
    heights = leg_ref.shape[1]
    mask = same_slot(sub, heights, levels)
    width = sub * 2
    north, south = [], []
    for first in range(0, step, sub):
        even, odd = split_parity(leg_ref, limit_ref, first, sub)
        spec = x_ref[:, pl.ds(first, sub)].reshape(levels * width, degrees)
        sums = []
        for table in (even, odd):
            cross = lax.dot_general(
                table, spec, (((1,), (1,)), ((), ())), preferred_element_type=jnp.float32
            ).reshape(sub, heights, levels * width)
            sums.append(jnp.sum(jnp.where(mask, cross, 0.0), axis=0))
        north.append(sums[0] + sums[1])
        south.append(sums[0] - sums[1])
    weight = weight_ref[...][:, :1]
    turn = turn_ref[...]
    bands = out_ref.shape[0]
    pairs = heights // bands
    for side, parts in enumerate((north, south)):
        total = None
        for level in range(levels + 1):
            if level < levels:
                lanes = slice(level * width, (level + 1) * width)
                value = jnp.concatenate([part[:, lanes] for part in parts], axis=1) * weight
                value = value * turn[0:1] + swap_pairs(value) * turn[1:2]
                total = value if total is None else total + value
            else:
                value = total
            sent = value.astype(jnp.bfloat16)
            for band in range(bands):
                rows = slice(level * pairs, (level + 1) * pairs)
                out_ref[band, side, rows] = sent[band * pairs : (band + 1) * pairs]


def analysis_kernel(step, sub, coef_ref, leg_ref, limit_ref, turn_ref, out_ref):
    levels, degrees = out_ref.shape[0], out_ref.shape[3]
    heights = leg_ref.shape[1]
    mask = same_slot(sub, heights, levels)
    width = sub * 2
    turn = turn_ref[...]
    held = coef_ref[...].astype(jnp.float32)
    bands = held.shape[0]
    pairs = heights // bands
    sides = []
    for side in range(2):
        values = []
        for level in range(levels):
            rows = slice(level * pairs, (level + 1) * pairs)
            value = jnp.concatenate([held[band, side, rows] for band in range(bands)], axis=0)
            values.append(value * turn[0:1] - swap_pairs(value) * turn[1:2])
        sides.append(values)
    for index, first in enumerate(range(0, step, sub)):
        tables = split_parity(leg_ref, limit_ref, first, sub)
        lanes = slice(index * width, (index + 1) * width)
        total = None
        for values, table in zip(sides, tables):
            row = jnp.concatenate([value[:, lanes] for value in values], axis=1)
            spread = jnp.where(mask, row[None], 0.0).reshape(sub * heights, levels * width)
            part = lax.dot_general(
                spread.astype(jnp.bfloat16),
                table,
                (((0,), (0,)), ((), ())),
                preferred_element_type=jnp.float32,
            )
            total = part if total is None else total + part
        out_ref[:, pl.ds(first, sub)] = total.astype(jnp.bfloat16).reshape(levels, sub, 2, degrees)


def spectral_call(kernel, slots, operands, specs, out_shape, out_spec, name):
    step, sub = slot_step(slots)
    return pl.pallas_call(
        functools.partial(kernel, step, sub),
        grid=(slots // step,),
        in_specs=specs,
        out_specs=out_spec,
        out_shape=out_shape,
        name=name,
        compiler_params=pltpu.CompilerParams(vmem_limit_bytes=48 * 1024 * 1024),
    )(*operands)


def cos_turn(count, period):
    left = count - jnp.floor(count * (1.0 / period)) * period
    angle = math.pi * (0.5 - jnp.abs(left * (2.0 / period) - 1.0))
    square = angle * angle
    series = 1.0
    for order in (11, 9, 7, 5, 3):
        series = 1.0 - series * square * (1.0 / (order * (order - 1)))
    return -angle * series


def trig_tables(waves, lon_count, width):
    quarter = lon_count // NBLK
    blocks = -(-quarter // LANES)
    period = 2 * lon_count
    wave = jnp.repeat(waves, 2).astype(jnp.float32)[:, None]
    shift = (jnp.arange(wave.shape[0], dtype=jnp.int32) % 2)[:, None] * (lon_count // 2)
    fine = wave * (2 * jnp.arange(LANES, dtype=jnp.int32) + 1).astype(jnp.float32)[None, :]
    coarse = wave * (2 * LANES * jnp.arange(blocks, dtype=jnp.int32)).astype(jnp.float32)[None, :]
    coarse = coarse + shift.astype(jnp.float32)
    quarter_back = 3.0 * (lon_count // 2)
    table = (
        cos_turn(coarse, period)[:, :, None] * cos_turn(fine, period)[:, None, :]
        - cos_turn(coarse + quarter_back, period)[:, :, None]
        * cos_turn(fine + quarter_back, period)[:, None, :]
    )
    return table.astype(jnp.bfloat16).reshape(wave.shape[0], blocks * LANES)


def body(adj_spec, wave_of_slot, legendre, lat_weight, traj, traj_exp, traj_order, lev_coef):
    levels, slots, _, degrees = adj_spec.shape
    heights = legendre.shape[1]
    lat_rows = traj.shape[1]
    pairs = lat_rows // 2
    lon_count = traj.shape[2]
    quarter = lon_count // NBLK
    norm_scale = 1.0 / math.sqrt(degrees)
    step, _ = slot_step(slots)
    bands = heights // pairs
    groups = lax.axis_size("lev")

    first_slot = lax.axis_index("band") * slots
    waves_here = lax.dynamic_slice_in_dim(wave_of_slot, first_slot, slots)
    limit = jnp.broadcast_to((degrees - waves_here)[:, None, None], (slots, heights, LANES))
    weight = jnp.broadcast_to(lat_weight[:, None], (heights, LANES))
    half_turn = jnp.repeat(waves_here, 2).astype(jnp.float32) * (math.pi / lon_count)
    part_sign = 1.0 - 2.0 * (jnp.arange(slots * 2, dtype=jnp.int32) % 2).astype(jnp.float32)
    turn = jnp.stack([jnp.cos(half_turn), jnp.sin(half_turn) * part_sign])

    spec_block = pl.BlockSpec((levels, step, 2, degrees), lambda i: (0, i, 0, 0))
    leg_block = pl.BlockSpec((step, heights, degrees), lambda i: (i, 0, 0))
    limit_block = pl.BlockSpec((step, heights, LANES), lambda i: (i, 0, 0))
    turn_block = pl.BlockSpec((2, step * 2), lambda i: (0, i))
    fourier = spectral_call(
        synthesis_kernel,
        slots,
        (adj_spec, legendre, limit, weight, turn),
        [spec_block, leg_block, limit_block, pl.BlockSpec((heights, LANES), lambda i: (0, 0)), turn_block],
        jax.ShapeDtypeStruct((bands, 2, (levels + 1) * pairs, slots * 2), jnp.bfloat16),
        pl.BlockSpec((bands, 2, (levels + 1) * pairs, step * 2), lambda i: (0, 0, 0, i)),
        "synthesis",
    )
    here = lax.all_to_all(fourier, "band", split_axis=0, concat_axis=0)
    totals = here[:, :, levels * pairs :]
    totals = jnp.broadcast_to(totals[None], (groups,) + totals.shape)
    totals = lax.all_to_all(totals, "lev", split_axis=0, concat_axis=0).astype(jnp.float32)
    group_ids = jnp.arange(groups, dtype=jnp.int32)
    earlier = (group_ids < lax.axis_index("lev"))[:, None, None, None, None]
    above = jnp.sum(jnp.where(earlier, totals, 0.0), axis=0)
    whole = []
    for level in range(levels):
        value = here[:, :, level * pairs : (level + 1) * pairs].astype(jnp.float32)
        whole.append(value + lev_coef[level] * above)
        above = above + value
    whole = jnp.concatenate(whole, axis=2).astype(jnp.bfloat16)
    rows = levels * lat_rows
    here = whole.transpose(1, 2, 0, 3).reshape(rows, -1)

    table = trig_tables(wave_of_slot, lon_count, quarter)
    padded = table.shape[1]
    one = jnp.ones((here.shape[1],), jnp.bfloat16)
    sign_c = jnp.where(jnp.arange(here.shape[1], dtype=jnp.int32) % 2 == 0, one, -one)
    sign_m = jnp.where(jnp.repeat(wave_of_slot, 2) % 2 == 0, one, -one)
    signs = jnp.stack([one, sign_m * sign_c, sign_m, sign_c])
    mirrored = (here[None] * signs[:, None, :]).reshape(NBLK * rows, -1)
    grid = jnp.dot(mirrored, table, preferred_element_type=jnp.float32) * norm_scale
    grid = grid.reshape(NBLK, rows, padded)

    stored = traj.reshape(levels, pairs, 2, NBLK, quarter).transpose(3, 0, 2, 1, 4)
    stored = jnp.stack([stored[0], stored[1, ..., ::-1], stored[2], stored[3, ..., ::-1]])
    scale = jnp.exp2(traj_exp.astype(jnp.float32))
    scale = scale.reshape(levels, pairs, 2, NBLK).transpose(3, 0, 2, 1)[..., None]
    scaled = (stored.astype(jnp.float32) * scale).reshape(NBLK, levels, lat_rows, quarter)
    order_ids = jnp.arange(levels, dtype=jnp.int32)
    select = traj_order[0][None, :] == order_ids[:, None]
    value = sum(
        jnp.where(select[:, r][None, :, None, None], scaled[:, r : r + 1], 0.0)
        for r in range(levels)
    )
    value = value.reshape(NBLK, levels, 2, pairs, quarter).transpose(0, 2, 1, 3, 4)
    value = value.reshape(NBLK, rows, quarter)
    gain = jnp.pad(1.0 + jnp.tanh(value), ((0, 0), (0, 0), (0, padded - quarter)))
    forcing = (gain * grid).astype(jnp.bfloat16).reshape(NBLK * rows, padded)
    back = lax.dot_general(
        forcing, table, (((1,), (1,)), ((), ())), preferred_element_type=jnp.float32
    ).reshape(NBLK, 2, levels * pairs, -1)
    back = jnp.sum(back * signs.astype(jnp.float32)[:, None, None, :], axis=0) * norm_scale
    both = jnp.stack([back[0] + back[1], back[0] - back[1]])
    both = both.astype(jnp.bfloat16)
    width = slots * 2
    both = jnp.stack([both[:, :, band * width : (band + 1) * width] for band in range(bands)])
    returned = lax.all_to_all(both, "band", split_axis=0, concat_axis=0)
    return spectral_call(
        analysis_kernel,
        slots,
        (returned, legendre, limit, turn),
        [pl.BlockSpec((bands, 2, levels * pairs, step * 2), lambda i: (0, 0, 0, i)), leg_block, limit_block, turn_block],
        jax.ShapeDtypeStruct(adj_spec.shape, jnp.bfloat16),
        spec_block,
        "analysis",
    )


def solution(mesh):
    placed = (
        P("lev", "band", None, None),
        P(),
        P("band", None, None),
        P(),
        P("lev", "band", None),
        P("lev", "band", None),
        P("lev", None),
        P("lev"),
    )
    return jax.shard_map(
        body, mesh=mesh, in_specs=placed, out_specs=P("lev", "band", None, None), check_vma=False
    )
```
